32 devices in a mesh: row: 8 (over y, x, core), col: 4 (over z).
Axes of the slice: x: 2, y: 2, z: 4, core: 2. Of those that a mesh axis runs over, the one named last changes fastest.
Arguments:
- gate_weight: bfloat16 [4096, 14336], P('row', 'col'), may hold values from -6 to 6
- up_weight: bfloat16 [4096, 14336], P('row', 'col'), may hold values from -6 to 6
- down_weight: bfloat16 [14336, 4096], P('row', 'col'), may hold values from -6 to 6
- gate_row_bits: int32 [4096], P('row'), may hold values from 0 to 1
- gate_col_bits: int32 [14336], P('col'), may hold values from 0 to 1
- up_row_bits: int32 [4096], P('row'), may hold values from 0 to 1
- up_col_bits: int32 [14336], P('col'), may hold values from 0 to 1
- down_row_bits: int32 [14336], P('row'), may hold values from 0 to 1
- down_col_bits: int32 [4096], P('col'), may hold values from 0 to 1
- block_order: int32 [7], replicated, may hold values from 0 to 6, each once
Outputs:
- gate_out: bfloat16 [4096, 14336], P('row', 'col')
- up_out: bfloat16 [4096, 14336], P('row', 'col')
- down_out: bfloat16 [14336, 4096], P('row', 'col')
The draws below stay inside these ranges and needn't reach their ends.
Inputs may be any that keep to these rules, and one draw needn't show every extreme that they name: block_order is a permutation of the 7 block numbers.
All inputs are finite; a program needn't handle non-finite values.
Results may differ from the reference program's by a relative error of at most 0.0013.
Values sent between devices are 32-bit elements; how exact they have to be, the bound alone decides.
No kernel may reach another device: no remote copies, remote signals or barrier semaphores. Data moves between devices by JAX's collectives and lax.ppermute only.
A program may use at most 128 MiB of HBM per device.

```python
import jax
import jax.numpy as jnp
from jax import lax

D = 4096
FF = 14336
BLK = 128
GROUPS = 16
HBLOCKS = 7


def touch_ends(values, rng, low, high):
    dims = values.shape
    spot = [jax.random.randint(jax.random.fold_in(rng, axis), (), 0, dims[axis]) for axis in range(len(dims))]
    values = values.at[tuple(spot)].set(low)
    longest = dims.index(max(dims))
    spot[longest] = (spot[longest] + 1) % dims[longest]
    return values.at[tuple(spot)].set(high)


def block_scale(key, extent, split, smallest, largest):
    loudness = 1.0
    for axis_at, blocks in split:
        draws = jax.random.uniform(jax.random.fold_in(jax.random.fold_in(key, 6), axis_at), (blocks,), jnp.float32, smallest / len(split), largest / len(split))
        loudness = loudness * jnp.repeat(jnp.exp(draws), extent[axis_at] // blocks).reshape((-1,) + (1,) * (len(extent) - 1 - axis_at))
    return loudness


def normal_values(key, extent, scale, limit, shards=(), dtype=jnp.bfloat16):
    array = scale * jax.random.normal(key, extent, jnp.float32)
    if shards:
        array = array * block_scale(key, extent, shards, -0.22, 0.18)
    return jnp.clip(array, -limit, limit).astype(dtype)


def setup_inputs(seed: int = 0) -> dict:
    splits = jax.random.split(jax.random.key(seed), 11)
    return {
        "gate_weight": normal_values(splits[0], (D, FF), 1.0, 6.0, ((0, 8), (1, 4))),
        "up_weight": normal_values(splits[1], (D, FF), 1.0, 6.0, ((0, 8), (1, 4))),
        "down_weight": normal_values(splits[2], (FF, D), 1.0, 6.0, ((0, 8), (1, 4))),
        "gate_row_bits": touch_ends(jax.random.randint(splits[3], (D,), 0, 2), jax.random.fold_in(splits[3], 1), 0, 1).astype(jnp.int32),
        "gate_col_bits": touch_ends(jax.random.randint(splits[4], (FF,), 0, 2), jax.random.fold_in(splits[4], 1), 0, 1).astype(jnp.int32),
        "up_row_bits": touch_ends(jax.random.randint(splits[5], (D,), 0, 2), jax.random.fold_in(splits[5], 1), 0, 1).astype(jnp.int32),
        "up_col_bits": touch_ends(jax.random.randint(splits[6], (FF,), 0, 2), jax.random.fold_in(splits[6], 1), 0, 1).astype(jnp.int32),
        "down_row_bits": touch_ends(jax.random.randint(splits[7], (FF,), 0, 2), jax.random.fold_in(splits[7], 1), 0, 1).astype(jnp.int32),
        "down_col_bits": touch_ends(jax.random.randint(splits[8], (D,), 0, 2), jax.random.fold_in(splits[8], 1), 0, 1).astype(jnp.int32),
        "block_order": jax.random.permutation(splits[9], HBLOCKS).astype(jnp.int32),
    }


HIGHEST = lax.Precision.HIGHEST


def sylvester(order_size):
    indices = lax.iota(jnp.int32, order_size)
    both = jnp.bitwise_and(indices[:, None], indices[None, :])
    folded = jnp.zeros_like(both)
    for shift in range(max(order_size.bit_length() - 1, 1)):
        folded = jnp.bitwise_xor(folded, jnp.right_shift(both, shift))
    parity = jnp.bitwise_and(folded, 1)
    return (1 - 2 * parity).astype(jnp.float32)


def split_sizes(order_size):
    exponent = order_size.bit_length() - 1
    leading = 1 << (exponent // 2)
    return leading, order_size // leading


def mix_model_rows(matrix):
    leading, trailing = split_sizes(matrix.shape[0])
    shaped = matrix.reshape(leading, trailing, matrix.shape[1])
    shaped = jnp.einsum('ab,bcm->acm', sylvester(leading), shaped, precision=HIGHEST)
    shaped = jnp.einsum('cd,adm->acm', sylvester(trailing), shaped, precision=HIGHEST)
    return shaped.reshape(matrix.shape)


def mix_model_cols(matrix):
    leading, trailing = split_sizes(matrix.shape[1])
    shaped = matrix.reshape(matrix.shape[0], leading, trailing)
    shaped = jnp.einsum('ab,mbc->mac', sylvester(leading), shaped, precision=HIGHEST)
    shaped = jnp.einsum('cd,mad->mac', sylvester(trailing), shaped, precision=HIGHEST)
    return shaped.reshape(matrix.shape)


def mix_hidden_cols(matrix, block_order):
    shaped = matrix.reshape(matrix.shape[0], GROUPS, HBLOCKS, BLK)
    shaped = jnp.einsum('gk,mkhb->mghb', sylvester(GROUPS), shaped, precision=HIGHEST)
    shaped = jnp.einsum('bc,mghc->mghb', sylvester(BLK), shaped, precision=HIGHEST)
    shaped = jnp.take(shaped, block_order, axis=2)
    return shaped.reshape(matrix.shape)


def mix_hidden_rows(matrix, block_order):
    shaped = matrix.reshape(GROUPS, HBLOCKS, BLK, matrix.shape[1])
    shaped = jnp.einsum('gk,khbm->ghbm', sylvester(GROUPS), shaped, precision=HIGHEST)
    shaped = jnp.einsum('bc,ghcm->ghbm', sylvester(BLK), shaped, precision=HIGHEST)
    shaped = jnp.take(shaped, block_order, axis=1)
    return shaped.reshape(matrix.shape)


def sign_values(sign_bits):
    return (1 - 2 * sign_bits).astype(jnp.float32)


def reference(gate_weight, up_weight, down_weight, gate_row_bits, gate_col_bits, up_row_bits, up_col_bits, down_row_bits, down_col_bits, block_order):
    factor = (D * GROUPS * BLK) ** -0.5

    def transform_in(weight, row_bits, col_bits):
        signed = weight.astype(jnp.float32) * sign_values(row_bits)[:, None] * sign_values(col_bits)[None, :]
        mixed = mix_hidden_cols(mix_model_rows(signed), block_order)
        return (mixed * factor).astype(jnp.bfloat16)

    signed = down_weight.astype(jnp.float32) * sign_values(down_row_bits)[:, None] * sign_values(down_col_bits)[None, :]
    mixed = mix_hidden_rows(mix_model_cols(signed), block_order)
    down_out = (mixed * factor).astype(jnp.bfloat16)
    gate_out = transform_in(gate_weight, gate_row_bits, gate_col_bits)
    up_out = transform_in(up_weight, up_row_bits, up_col_bits)
    return gate_out, up_out, down_out
```

```python
import functools

import jax
import jax.numpy as jnp
from jax import lax
from jax.experimental import pallas as pl
from jax.experimental.pallas import tpu as pltpu
from jax.sharding import PartitionSpec as P

BLK = 128
GROUPS = 16
HBLOCKS = 7


def sylvester(order_size, indices):
    both = jnp.bitwise_and(indices[:, None], indices[None, :])
    folded = jnp.zeros_like(both)
    for shift in range(max(order_size.bit_length() - 1, 1)):
        folded = jnp.bitwise_xor(folded, jnp.right_shift(both, shift))
    return (1 - 2 * jnp.bitwise_and(folded, 1)).astype(jnp.bfloat16)


def tie(value, after):
    if not after:
        return value
    return lax.optimization_barrier((value, *after))[0]


def exchange(value, axis, mask):
    size = lax.axis_size(axis)
    return lax.ppermute(value, axis, [(i, i ^ mask) for i in range(size)])


def signed(block_ref, row_ref, col_ref):
    width = block_ref.shape[1]
    parts = [
        block_ref[:, at : at + BLK].astype(jnp.float32) * row_ref[...] * col_ref[:, at : at + BLK]
        for at in range(0, width, BLK)
    ]
    return parts


def tiles_of(rows):
    return min(rows, 128)


def dot(a, b):
    return jnp.dot(a, b, preferred_element_type=jnp.float32)


def halves(value):
    high = value.astype(jnp.bfloat16)
    return high, (value - high.astype(jnp.float32)).astype(jnp.bfloat16)


class Matrix:
    def __init__(self, weight, row_bits, col_bits, hidden_axis, order):
        self.weight, self.hidden_axis, self.order = weight, hidden_axis, order
        rows, cols = weight.shape
        self.shape = weight.shape
        self.groups = weight.shape[hidden_axis] // (HBLOCKS * BLK)
        self.row_sign = jnp.broadcast_to((1 - 2 * row_bits).astype(jnp.float32)[:, None], (rows, BLK))
        self.col_sign = (1 - 2 * col_bits).astype(jnp.float32)[None, :]
        self.block = (rows, BLK) if hidden_axis else (BLK, cols)
        self.piece = (rows, self.groups * BLK) if hidden_axis else (self.groups * BLK, cols)
        self.out = None

    def at(self, index):
        return (0, index) if self.hidden_axis else (index, 0)

    def in_specs(self, h, group=None):
        def index(*ids):
            g = ids[0] if group is None else group
            return g * HBLOCKS + ids[-1][h]

        row_block = self.block[0]
        specs = [pl.BlockSpec(self.block, lambda *ids: self.at(index(*ids)))]
        specs.append(pl.BlockSpec((row_block, BLK), lambda *ids: (0, 0) if self.hidden_axis else (index(*ids), 0)))
        specs.append(pl.BlockSpec((1, self.block[1]), lambda *ids: (0, index(*ids)) if self.hidden_axis else (0, 0)))
        return specs

    def cost(self, flops):
        size = self.piece[0] * self.piece[1]
        return pl.CostEstimate(flops=max(flops, 8 * size), bytes_accessed=12 * size, transcendentals=0)

    def raw(self, h, order):
        def body(order_ref, block_ref, row_ref, col_ref, out_ref):
            for n, part in enumerate(signed(block_ref, row_ref, col_ref)):
                out_ref[:, n * BLK : (n + 1) * BLK] = part

        return pl.pallas_call(
            body,
            grid_spec=pltpu.PrefetchScalarGridSpec(
                num_scalar_prefetch=1,
                grid=(self.groups,),
                in_specs=self.in_specs(h),
                out_specs=pl.BlockSpec(self.block, lambda g, order: self.at(g)),
            ),
            out_shape=jax.ShapeDtypeStruct(self.piece, jnp.float32),
            cost_estimate=self.cost(0),
            name="raw",
        )(order, self.weight, self.row_sign, self.col_sign)

    def mixed(self, h, order, hadamard):
        rows, cols = self.piece
        step = tiles_of(rows)

        def body(order_ref, *refs):
            left_ref, right_ref = refs[3 * self.groups : 3 * self.groups + 2]
            out_ref, first, high, low = refs[3 * self.groups + 2 :]
            for g in range(self.groups):
                for n, part in enumerate(signed(*refs[3 * g : 3 * g + 3])):
                    part = part.astype(jnp.bfloat16)
                    if self.hidden_axis:
                        first[:, g * BLK : (g + 1) * BLK] = part
                    else:
                        first[g * BLK : (g + 1) * BLK, n * BLK : (n + 1) * BLK] = part

            def across(t, carry):
                at = pl.ds(pl.multiple_of(t * step, step), step)
                high[at, :], low[at, :] = halves(dot(first[at, :], right_ref[...]))
                return carry

            def down(t, carry):
                at = pl.ds(pl.multiple_of(t * step, step), step)
                out_ref[at, :] = dot(left_ref[at, :], high[...]) + dot(left_ref[at, :], low[...])
                return carry

            lax.fori_loop(0, rows // step, across, 0)
            lax.fori_loop(0, rows // step, down, 0)

        specs, operands = [], []
        for g in range(self.groups):
            specs += self.in_specs(h, g)
            operands += [self.weight, self.row_sign, self.col_sign]
        specs.append(pl.BlockSpec((rows, rows), lambda i, order: (0, 0)))
        specs.append(pl.BlockSpec((cols, cols), lambda i, order: (0, 0)))
        return pl.pallas_call(
            body,
            grid_spec=pltpu.PrefetchScalarGridSpec(
                num_scalar_prefetch=1,
                grid=(1,),
                in_specs=specs,
                out_specs=pl.BlockSpec(self.piece, lambda i, order: (0, 0)),
                scratch_shapes=[pltpu.VMEM(self.piece, jnp.bfloat16)] * 3,
            ),
            out_shape=jax.ShapeDtypeStruct(self.piece, jnp.float32),
            cost_estimate=self.cost(2 * rows * cols * (cols + 2 * rows)),
            name="mixed",
        )(order, *operands, hadamard, hadamard)

    def finish(self, h, factor, sign, mine, theirs, hadamard=None):
        rows, cols = self.piece
        step = tiles_of(rows)

        def plain(sign_ref, mine_ref, theirs_ref, *refs):
            out_ref = refs[-1]
            out_ref[...] = ((theirs_ref[...] + sign_ref[0] * mine_ref[...]) * factor).astype(jnp.bfloat16)

        def mixing(sign_ref, mine_ref, theirs_ref, left_ref, right_ref, *refs):
            out_ref, result, high, low = refs[-4:]
            group = pl.program_id(0)

            @pl.when(group == 0)
            def _():
                def across(t, carry):
                    at = pl.ds(pl.multiple_of(t * step, step), step)
                    top, rest = halves(theirs_ref[at, :] + sign_ref[0] * mine_ref[at, :])
                    high[at, :], low[at, :] = halves(dot(top, right_ref[...]) + dot(rest, right_ref[...]))
                    return carry

                def down(t, carry):
                    at = pl.ds(pl.multiple_of(t * step, step), step)
                    value = dot(left_ref[at, :], high[...]) + dot(left_ref[at, :], low[...])
                    value = (value * factor).astype(jnp.bfloat16)
                    for g in range(self.groups):
                        if self.hidden_axis:
                            result[g, at, :] = value[:, g * BLK : (g + 1) * BLK]
                    if not self.hidden_axis:
                        result[t] = value
                    return carry

                lax.fori_loop(0, rows // step, across, 0)
                lax.fori_loop(0, rows // step, down, 0)

            out_ref[...] = result[group]

        if hadamard is None:
            body, flops, scratch, more = plain, 0, [], []
            specs = [pl.BlockSpec(self.block, lambda g, sign: self.at(g))] * 2
        else:
            body, flops = mixing, 4 * rows * cols * (rows + cols)
            specs = [pl.BlockSpec(self.piece, lambda g, sign: (0, 0))] * 2
            specs.append(pl.BlockSpec((rows, rows), lambda g, sign: (0, 0)))
            specs.append(pl.BlockSpec((cols, cols), lambda g, sign: (0, 0)))
            more = [hadamard, hadamard]
            scratch = [pltpu.VMEM((self.groups, *self.block), jnp.bfloat16)]
            scratch += [pltpu.VMEM(self.piece, jnp.bfloat16)] * 2
        aliases = {}
        if self.out is not None:
            specs.append(pl.BlockSpec(memory_space=pl.ANY))
            more.append(self.out)
            aliases = {len(specs): 0}
        self.out = pl.pallas_call(
            body,
            grid_spec=pltpu.PrefetchScalarGridSpec(
                num_scalar_prefetch=1,
                grid=(self.groups,),
                in_specs=specs,
                out_specs=pl.BlockSpec(self.block, lambda g, sign: self.at(g * HBLOCKS + h)),
                scratch_shapes=scratch,
            ),
            out_shape=jax.ShapeDtypeStruct(self.shape, jnp.bfloat16),
            input_output_aliases=aliases,
            cost_estimate=self.cost(flops),
            name="finish",
        )(sign, mine, theirs, *more)


def on_device(
    gate_weight,
    up_weight,
    down_weight,
    gate_row_bits,
    gate_col_bits,
    up_row_bits,
    up_col_bits,
    down_row_bits,
    down_col_bits,
    order,
):
    row_size, col_size = lax.axis_size("row"), lax.axis_size("col")
    row_at, col_at = lax.axis_index("row"), lax.axis_index("col")
    gate = Matrix(gate_weight, gate_row_bits, gate_col_bits, 1, order)
    up = Matrix(up_weight, up_row_bits, up_col_bits, 1, order)
    down = Matrix(down_weight, down_row_bits, down_col_bits, 0, order)
    factor = (gate_weight.shape[0] * row_size * GROUPS * BLK) ** -0.5

    def sign_at(axis, mask):
        index = row_at if axis == "row" else col_at
        return 1.0 - 2.0 * (jnp.bitwise_and(index, mask) != 0).astype(jnp.float32)

    def powers(size):
        return [1 << bit for bit in range(size.bit_length() - 1)]

    relay = col_size == 4
    row_stages = [("row", mask) for mask in reversed(powers(row_size))]
    col_stages = [("col", mask) for mask in powers(col_size)]
    cross = col_stages.pop()
    early_stages = row_stages + col_stages
    late_stages = row_stages if relay else col_stages + row_stages

    pieces = [(m, h) for m in (gate, up, down) for h in range(HBLOCKS)]
    n_first = (len(pieces) + 1) // 2
    first, last = pieces[:n_first], pieces[n_first:]
    total = len(pieces)

    middle = jnp.logical_and(col_at > 0, col_at < col_size - 1)
    lower = 1.0 - 2.0 * (col_at >= col_size // 2).astype(jnp.float32)

    crossed = {}

    def when(k):
        return crossed.get(k - 1, ())

    def stage(value, which, k):
        value = tie(value, when(k))
        return value, exchange(value, *which)

    def add(which, mine, theirs):
        return theirs + sign_at(*which) * mine

    raws, inward = {}, {}

    def prepare(k):
        if k < n_first:
            m, h = first[k]
            raws[k] = m.raw(h, tie(order, when(k - 2)))
            if relay:
                inward[k] = lax.ppermute(tie(raws[k], when(k - 1)), "col", [(0, 1), (3, 2)])

    state = {}
    hadamard_box = []

    def hadamard():
        return hadamard_box[0]

    across = [(1, 2), (2, 1)]
    prepare(0)
    prepare(1)
    largest = max(max(m.piece) for m in (gate, down))
    indices = tie(lax.iota(jnp.int32, largest), (raws[0], raws[1]))
    hadamard_box.append(sylvester(largest, indices))

    late_start = total - n_first - len(late_stages)
    after_cross = {}
    ready = {}
    early = {}
    late = {}
    backward = {}

    def start_cross(k):
        if k < n_first:
            if relay:
                own = tie(raws[k], when(k - 1))
                leaf = tie(inward[k], when(k - 1))
                crossed[k] = (lax.ppermute(own, "col", across), lax.ppermute(leaf, "col", across))
                after_cross[k] = (own, leaf)
            else:
                own, theirs = stage(raws[k], cross, k - 1)
                crossed[k] = (theirs,)
                after_cross[k] = (own,)
        else:
            own, theirs = stage(ready[k - n_first], cross, k - 1)
            crossed[k] = (theirs,)
            after_cross[k] = (own,)

    start_cross(0)
    start_cross(1)
    for k in range(total + 1):
        prepare(k + 2)
        for j in range(len(last)):
            s = k - j
            if s == 0:
                m, h = last[j]
                early[j] = stage(m.mixed(h, tie(order, when(k)), hadamard()), early_stages[0], k)
            elif 0 < s < len(early_stages):
                early[j] = stage(add(early_stages[s - 1], *early[j]), early_stages[s], k)
            elif s == len(early_stages):
                ready[j] = add(early_stages[-1], *early[j])
        j = k - 1
        if 0 <= j < n_first:
            if relay:
                own, leaf = after_cross[j]
                their_own, their_leaf = crossed[j]
                keep = their_own - own + lower * (leaf - their_leaf)
                give = leaf + their_leaf + lower * (own + their_own)
                backward[j] = (keep, lax.ppermute(give, "col", [(1, 0), (2, 3)]))
            else:
                backward[j] = (after_cross[j][0], crossed[j][0])
        for j in range(n_first):
            s = k - max(late_start, 2) - j
            if s == 0:
                if relay:
                    value = jnp.where(middle, *backward[j])
                else:
                    value = add(cross, *backward[j])
                late[j] = stage(value, late_stages[0], k)
            elif 0 < s < len(late_stages):
                late[j] = stage(add(late_stages[s - 1], *late[j]), late_stages[s], k)
            elif s == len(late_stages):
                m, h = first[j]
                m.finish(h, factor, sign_at(*late_stages[-1])[None], *late[j], hadamard())
        j = k - 1
        if j >= n_first:
            m, h = pieces[j]
            m.finish(h, factor, sign_at(*cross)[None], after_cross[j][0], crossed[j][0])
        if 1 <= k and k + 1 < total:
            start_cross(k + 1)
    return gate.out, up.out, down.out


def solution(mesh):
    return jax.shard_map(
        on_device,
        mesh=mesh,
        in_specs=(
            P("row", "col"),
            P("row", "col"),
            P("row", "col"),
            P("row"),
            P("col"),
            P("row"),
            P("col"),
            P("row"),
            P("col"),
            P(),
        ),
        out_specs=(P("row", "col"), P("row", "col"), P("row", "col")),
        check_vma=False,
    )
```
